32 devices in a mesh: gx: 2 (over y), gy: 4 (over z), gz: 4 (over x, core).
Axes of the slice: x: 2, y: 2, z: 4, core: 2. Of those that a mesh axis runs over, the one named last changes fastest.
Arguments:
- concentration: float32 [32, 256, 512], P('gx', 'gy', 'gz'), may hold values from -6 to 6
- speed: float32 [3, 32, 256, 512], P(None, 'gx', 'gy', 'gz'), may hold values from 0.1 to 1
- signs: int32 [3, 32, 256, 512], P(None, 'gx', 'gy', 'gz'), may hold values from 0 to 1
- diffusivity: float32 [32, 256, 512], P('gx', 'gy', 'gz'), may hold values from 0.02 to 0.12
- shear: int32 [1], replicated, may hold values from 0 to 255
Outputs:
- final_field: float32 [32, 256, 512], P('gx', 'gy', 'gz')
The draws below stay inside these ranges and needn't reach their ends.
All inputs are finite; a program needn't handle non-finite values.
Results may differ from the reference program's by a relative error of at most 0.00002.
Values sent between devices are 32-bit elements; how exact they have to be, the bound alone decides.
A program may use at most 64 MiB of HBM per device.

```python
import math
import jax
import jax.numpy as jnp

STEPS = 8
NX = 32
NY = 256
NZ = 512


def with_ends(values, rng, low, largest):
    shape = values.shape
    place = [jax.random.randint(jax.random.fold_in(rng, axis), (), 0, shape[axis]) for axis in range(len(shape))]
    values = values.at[tuple(place)].set(low)
    longest = shape.index(max(shape))
    place[longest] = (place[longest] + 1) % shape[longest]
    return values.at[tuple(place)].set(largest)


def level_of(rng, shape, shards, least, high):
    loudness, own = 1.0, jax.random.fold_in(rng, 6)
    for position, parts in shards:
        draws = jnp.exp(jax.random.uniform(jax.random.fold_in(own, position), (parts,), jnp.float32, least / len(shards), high / len(shards)))
        loudness = loudness * jnp.repeat(draws, shape[position] // parts).reshape([-1 if axis == position else 1 for axis in range(len(shape))])
    return loudness


def scatter_about(own_key, dims, width, limit, pieces=(), kind=jnp.bfloat16):
    entries = width * jax.random.normal(own_key, dims, jnp.float32)
    if pieces:
        entries = entries * level_of(own_key, dims, pieces, -0.22, 0.18)
    return jnp.clip(entries, -limit, limit).astype(kind)


def setup_inputs(seed: int = 0) -> dict:
    key_list = jax.random.split(jax.random.key(seed), 6)
    concentration = scatter_about(key_list[0], (NX, NY, NZ), 1.0, 6.0, ((0, 2), (1, 4), (2, 4)), jnp.float32)
    speed = jnp.clip(jnp.exp(math.log(1.0) - 2.3025851 * jax.random.uniform(key_list[1], (3, NX, NY, NZ), jnp.float32) ** level_of(key_list[1], (3, NX, NY, NZ), ((1, 2), (2, 4), (3, 4)), -0.2, 0.2)), 0.1, 1.0)
    signs = with_ends(jax.random.randint(key_list[2], (3, NX, NY, NZ), 0, 2), jax.random.fold_in(key_list[2], 1), 0, 1).astype(jnp.int32)
    diffusivity = jnp.clip(jnp.exp(math.log(0.12) - 1.7917595 * jax.random.uniform(key_list[3], (NX, NY, NZ), jnp.float32) ** level_of(key_list[3], (NX, NY, NZ), ((0, 2), (1, 4), (2, 4)), -0.2, 0.2)), 0.02, 0.12)
    shear = jax.random.randint(key_list[4], (1,), 0, NY).astype(jnp.int32)
    return {"concentration": concentration, "speed": speed, "signs": signs, "diffusivity": diffusivity, "shear": shear}


time_step = 0.25


def advance(field, neighbours, speed, signs, diffusivity):
    total = jnp.zeros_like(field)
    for axis_id in range(3):
        below, above = neighbours[axis_id]
        upwind = jnp.where(signs[axis_id] > 0, field - below, above - field)
        total = total + diffusivity * (above + below - 2.0 * field) - speed[axis_id] * upwind
    return field + time_step * total


def reference(concentration, speed, signs, diffusivity, shear):
    offset = shear[0]
    field = concentration
    for step in range(STEPS):
        lower = jnp.roll(field[-1], -offset, axis=0)
        upper = jnp.roll(field[0], offset, axis=0)
        x_minus = jnp.concatenate([lower[None], field[:-1]], axis=0)
        x_plus = jnp.concatenate([field[1:], upper[None]], axis=0)
        y_minus = jnp.roll(field, 1, axis=1)
        y_plus = jnp.roll(field, -1, axis=1)
        z_minus = jnp.roll(field, 1, axis=2)
        z_plus = jnp.roll(field, -1, axis=2)
        field = advance(field, ((x_minus, x_plus), (y_minus, y_plus), (z_minus, z_plus)), speed, signs, diffusivity)
    return field
```

```python
import functools

import jax
import jax.numpy as jnp
from jax import lax
from jax.experimental import pallas as pl
from jax.experimental.pallas import tpu as pltpu
from jax.sharding import PartitionSpec as P

STEPS = 8
time_step = 0.25
PAD = 8
MESH = pl.DeviceIdType.MESH


def kernel(
    hops, count_x, count_y, count_z,
    shear, conc, speed, signs, diff, out,
    field0, field1, coef, v_buf, s_buf, d_buf, low0, low1, high0, high1,
    y_out0, y_out1, y_in0, y_in1, z_out0, z_out1, z_in0, z_in1,
    load_sem, send_sem, recv_sem,
):
    nx, rows, lanes = conc.shape
    blocks = rows // 8
    span = 2 * nx
    per = lanes // span
    gx, gy, gz = (lax.axis_index(name) for name in ("gx", "gy", "gz"))
    low, high, field = (low0, low1), (high0, high1), (field0, field1)
    y_out, y_in = (y_out0, y_out1), (y_in0, y_in1)
    z_out, z_in = (z_out0, z_out1), (z_in0, z_in1)
    first, last = gx == 0, gx == count_x - 1
    body_rows = pl.ds(PAD, rows)

    def at(x, y):
        return {"gx": x, "gy": lax.rem(y + 2 * count_y, count_y)}

    up = (
        at(jnp.where(last, 0, gx + 1), gy - jnp.where(last, hops, 0)),
        at(0, gy - hops - 1),
    )
    down = (
        at(jnp.where(first, count_x - 1, gx - 1), gy + jnp.where(first, hops + 1, 0)),
        at(count_x - 1, gy + hops),
    )
    before_y, after_y = at(gx, gy - 1), at(gx, gy + 1)
    before_z = {"gz": lax.rem(gz + count_z - 1, count_z)}
    after_z = {"gz": lax.rem(gz + 1, count_z)}

    def remote(p, role, source, target, device):
        return pltpu.make_async_remote_copy(
            src_ref=source, dst_ref=target,
            send_sem=send_sem.at[p, role], recv_sem=recv_sem.at[p, role],
            device_id=device, device_id_type=MESH,
        )

    def copies(p):
        top = field[p].at[nx - 1, body_rows]
        bottom = field[p].at[0, body_rows]
        halves = (pl.ds(0, rows), pl.ds(rows, rows))
        return (
            remote(p, 0, top, low[p].at[halves[0]], up[0]),
            remote(p, 1, top, low[p].at[halves[1]], up[1]),
            remote(p, 2, bottom, high[p].at[halves[0]], down[0]),
            remote(p, 3, bottom, high[p].at[halves[1]], down[1]),
            remote(p, 4, y_out[p].at[0], y_in[p].at[1], before_y),
            remote(p, 5, y_out[p].at[1], y_in[p].at[0], after_y),
            remote(p, 6, z_out[p], z_in[p].at[1], before_z),
            remote(p, 7, z_out[p], z_in[p].at[0], after_z),
        )

    def send(p):
        c = copies(p)
        pl.when(last)(c[1].start)
        pl.when(first)(c[3].start)
        for role in (0, 2, 4, 5, 6, 7):
            c[role].start()

    lane = lax.broadcasted_iota(jnp.int32, (8, lanes), 1)
    even = lane % 2 == 0

    def turn(value, amount):
        amount = amount % lanes
        return pltpu.roll(value, amount, 1) if amount else value

    def record(q, packed, block, x, value):
        spot = span * (block % per) + 2 * x
        group = block // per
        moved = turn(value, spot + 1)
        packed[group] = jnp.where((lane == spot) | (lane == spot + 1), moved, packed[group])
        if block == 0:
            y_out[q][0, pl.ds(x, 1)] = value[:1]
        if block == blocks - 1:
            y_out[q][1, pl.ds(x, 1)] = value[7:]

    def store_packed(q, packed):
        for group, value in enumerate(packed):
            z_out[q][group] = value

    groups = blocks // per
    def nothing():
        return [jnp.zeros((8, lanes), jnp.float32) for _ in range(groups)]

    loads = (
        pltpu.make_async_copy(conc, field[0].at[:, body_rows], load_sem.at[0]),
        pltpu.make_async_copy(diff, d_buf, load_sem.at[1]),
        pltpu.make_async_copy(speed, v_buf, load_sem.at[2]),
        pltpu.make_async_copy(signs, s_buf, load_sem.at[3]),
    )
    for load in loads:
        load.start()

    barrier = pltpu.get_barrier_semaphore()

    def greet(device):
        pl.semaphore_signal(barrier, inc=1, device_id=device, device_id_type=MESH)

    for device in (up[0], down[0], before_y, after_y, before_z, after_z):
        greet(device)
    pl.when(last)(lambda: greet(up[1]))
    pl.when(first)(lambda: greet(down[1]))
    pl.semaphore_wait(barrier, 6 + jnp.where(first | last, 1, 0))

    loads[0].wait()

    packed = nothing()
    for block in range(blocks):
        for x in range(nx):
            record(0, packed, block, x, field[0][x, pl.ds(PAD + 8 * block, 8)])
    store_packed(0, packed)
    send(0)
    for load in loads[1:]:
        load.wait()

    def weigh(x, carry):
        d = time_step * d_buf[x]
        centre = 1.0 - 6.0 * d
        for axis in range(3):
            v = time_step * v_buf[axis, x]
            forward = s_buf[axis, x] > 0
            below = jnp.where(forward, v, 0.0)
            above = v - below
            coef[1 + 2 * axis, x] = d + below
            coef[2 + 2 * axis, x] = d - above
            centre = centre - below + above
        coef[0, x] = centre
        return carry

    lax.fori_loop(0, nx, weigh, 0)

    residue = lax.rem(shear[0], rows)
    low_start = jnp.where(first, residue, 0)
    high_start = jnp.where(last, rows - residue, 0)

    def step(p, more):
        q = 1 - p
        c = copies(p)
        old, new = field[p], field[q]
        c[6].wait_recv()
        c[7].wait_recv()
        sides = [
            jnp.where(even, z_in[p][0, group], turn(z_in[p][1, group], -2))
            for group in range(groups)
        ]

        def cells(block, x, lower, here, upper):
            start = PAD + 8 * block
            part = pl.ds(8 * block, 8)
            side = turn(sides[block // per], -(span * (block % per) + 2 * x))
            z_minus = jnp.where(lane == 0, side, turn(here, 1))
            z_plus = jnp.where(lane == lanes - 1, side, turn(here, -1))
            total = (
                (coef[0, x, part] * here + coef[1, x, part] * lower)
                + (coef[2, x, part] * upper
                   + coef[3, x, part] * old[x, pl.ds(start - 1, 8)])
            ) + (
                (coef[4, x, part] * old[x, pl.ds(start + 1, 8)]
                 + coef[5, x, part] * z_minus)
                + coef[6, x, part] * z_plus
            )
            new[x, pl.ds(start, 8)] = total

        def column(block):
            at_x = lambda x: old[x, pl.ds(PAD + 8 * block, 8)]
            lower, here = at_x(0), at_x(1)
            for x in range(1, nx - 1):
                upper = at_x(x + 1)
                cells(block, x, lower, here, upper)
                lower, here = here, upper

        for block in range(1, blocks - 1):
            column(block)
        c[4].wait_recv()
        c[5].wait_recv()
        for x in range(nx):
            old[x, pl.ds(PAD - 1, 1)] = y_in[p][0, pl.ds(x, 1)]
            old[x, pl.ds(PAD + rows, 1)] = y_in[p][1, pl.ds(x, 1)]
        column(0)
        column(blocks - 1)
        c[0].wait_recv()
        c[2].wait_recv()
        pl.when(first)(c[1].wait_recv)
        pl.when(last)(c[3].wait_recv)
        for block in range(blocks):
            at_x = lambda x: old[x, pl.ds(PAD + 8 * block, 8)]
            cells(block, 0, low[p][pl.ds(low_start + 8 * block, 8)], at_x(0), at_x(1))
            cells(block, nx - 1, at_x(nx - 2), at_x(nx - 1), high[p][pl.ds(high_start + 8 * block, 8)])
        packed = nothing()
        for block in range(blocks):
            for x in range(nx):
                record(q, packed, block, x, new[x, pl.ds(PAD + 8 * block, 8)])
        store_packed(q, packed)
        for role in (0, 2, 4, 5, 6, 7):
            c[role].wait_send()
        pl.when(last)(c[1].wait_send)
        pl.when(first)(c[3].wait_send)
        if more is None:
            send(q)
        else:
            pl.when(more)(lambda: send(q))

    def pair(t, carry):
        step(0, None)
        step(1, t < STEPS // 2 - 1)
        return carry

    lax.fori_loop(0, STEPS // 2, pair, 0)
    store = pltpu.make_async_copy(field[STEPS % 2].at[:, body_rows], out, load_sem.at[0])
    store.start()
    store.wait()


def run(hops, counts, shear, conc, speed, signs, diff):
    nx, rows, lanes = conc.shape
    f32 = jnp.float32
    groups = (rows // 8) // (lanes // (2 * nx))
    anywhere = pl.BlockSpec(memory_space=pl.ANY)
    return pl.pallas_call(
        functools.partial(kernel, hops, *counts),
        name=f"slide{hops}",
        out_shape=jax.ShapeDtypeStruct(conc.shape, f32),
        in_specs=[pl.BlockSpec(memory_space=pltpu.SMEM)] + [anywhere] * 4,
        out_specs=anywhere,
        scratch_shapes=[
            pltpu.VMEM((nx, rows + 2 * PAD, lanes), f32),
            pltpu.VMEM((nx, rows + 2 * PAD, lanes), f32),
            pltpu.VMEM((7, nx, rows, lanes), f32),
            pltpu.VMEM((3, nx, rows, lanes), f32),
            pltpu.VMEM((3, nx, rows, lanes), jnp.int32),
            pltpu.VMEM((nx, rows, lanes), f32),
            pltpu.VMEM((2 * rows, lanes), f32),
            pltpu.VMEM((2 * rows, lanes), f32),
            pltpu.VMEM((2 * rows, lanes), f32),
            pltpu.VMEM((2 * rows, lanes), f32),
            *[pltpu.VMEM((2, nx, lanes), f32)] * 4,
            *[pltpu.VMEM((groups, 8, lanes), f32)] * 2,
            *[pltpu.VMEM((2, groups, 8, lanes), f32)] * 2,
            pltpu.SemaphoreType.DMA((4,)),
            pltpu.SemaphoreType.DMA((2, 8)),
            pltpu.SemaphoreType.DMA((2, 8)),
        ],
        compiler_params=pltpu.CompilerParams(collective_id=hops, has_side_effects=True),
    )(shear, conc, speed, signs, diff)


def body(concentration, speed, signs, diffusivity, shear):
    counts = tuple(lax.axis_size(name) for name in ("gx", "gy", "gz"))
    rows = concentration.shape[1]
    branches = [functools.partial(run, hops, counts) for hops in range(counts[1])]
    return lax.switch(
        lax.div(shear[0], rows), branches, shear, concentration, speed, signs, diffusivity
    )


def solution(mesh):
    placed = (
        P("gx", "gy", "gz"),
        P(None, "gx", "gy", "gz"),
        P(None, "gx", "gy", "gz"),
        P("gx", "gy", "gz"),
        P(),
    )
    return jax.shard_map(
        body, mesh=mesh, in_specs=placed, out_specs=P("gx", "gy", "gz"), check_vma=False
    )
```

```python
import functools

import jax
import jax.numpy as jnp
from jax import lax
from jax.experimental import pallas as pl
from jax.experimental.pallas import tpu as pltpu
from jax.sharding import PartitionSpec as P

STEPS = 8
time_step = 0.25
PAD = 8
TURNS = 4
BUCKETS = 2
MESH = pl.DeviceIdType.MESH


def kernel(
    hops, aligned, floor, width, count_x, count_y, count_z,
    shear, conc, speed, signs, diff, out,
    field, coef, v_buf, s_buf, d_buf, part, x_in, window, halo, xc_out, xc_in,
    y_out, y_in, yc_out, yc_in, own_y, z_out, z_in,
    load_sem, send_sem, recv_sem, coef_send, coef_recv,
):
    nx, rows, lanes = conc.shape
    blocks = rows // 8
    span = 2 * nx
    per = lanes // span
    groups = blocks // per
    ends = (0, nx - 1)
    gx, gy, gz = (lax.axis_index(name) for name in ("gx", "gy", "gz"))
    first, last = gx == 0, gx == count_x - 1
    not_first, not_last = gx != 0, gx != count_x - 1
    body_rows = pl.ds(PAD, rows)

    def at(x, y):
        return {"gx": x, "gy": lax.rem(y + 2 * count_y, count_y)}

    more = 0 if aligned else 1
    up = (
        at(jnp.where(last, 0, gx + 1), gy - jnp.where(last, hops, 0)),
        at(0, gy - hops - 1),
    )
    down = (
        at(jnp.where(first, count_x - 1, gx - 1), gy + jnp.where(first, hops + more, 0)),
        at(count_x - 1, gy + hops),
    )
    before_y, after_y = at(gx, gy - 1), at(gx, gy + 1)
    before_z = {"gz": lax.rem(gz + count_z - 1, count_z)}
    after_z = {"gz": lax.rem(gz + 1, count_z)}

    def remote(t, role, source, target, device):
        return pltpu.make_async_remote_copy(
            src_ref=source, dst_ref=target,
            send_sem=send_sem.at[t % TURNS, role], recv_sem=recv_sem.at[t % TURNS, role],
            device_id=device, device_id_type=MESH,
        )

    ceiling = floor + width

    def over_planes(t, top, bottom):
        if aligned:
            return (
                remote(t, 0, top(0, rows), x_in.at[t, 0, pl.ds(0, rows)], up[0]), None,
                remote(t, 2, bottom(0, rows), x_in.at[t, 1, pl.ds(0, rows)], down[0]), None,
            )
        far, near = rows - ceiling, rows - floor
        return (
            remote(t, 0, top(floor, near), x_in.at[t, 0, pl.ds(floor, near)], up[0]),
            remote(t, 1, top(0, ceiling), x_in.at[t, 0, pl.ds(rows, ceiling)], up[1]),
            remote(t, 2, bottom(far, ceiling), x_in.at[t, 1, pl.ds(far, ceiling)], down[0]),
            remote(t, 3, bottom(0, near), x_in.at[t, 1, pl.ds(rows, near)], down[1]),
        )

    def field_over(t, p):
        return over_planes(
            t,
            lambda a, n: field.at[p, nx - 1, pl.ds(PAD + a, n)],
            lambda a, n: field.at[p, 0, pl.ds(PAD + a, n)],
        )

    def part_over(t):
        return over_planes(
            t, lambda a, n: part.at[t, 1, pl.ds(a, n)], lambda a, n: part.at[t, 0, pl.ds(a, n)]
        )

    def inside_planes(t, p):
        return (
            remote(t, 0, field.at[p, nx - 1, body_rows], x_in.at[t, 0, pl.ds(0, rows)], up[0]),
            remote(t, 2, field.at[p, 0, body_rows], x_in.at[t, 1, pl.ds(0, rows)], down[0]),
        )

    def edges(t):
        return (
            remote(t, 4, y_out.at[t, 0], y_in.at[t, 1], before_y),
            remote(t, 5, y_out.at[t, 1], y_in.at[t, 0], after_y),
            remote(t, 6, z_out.at[t], z_in.at[t, 1], before_z),
            remote(t, 7, z_out.at[t], z_in.at[t, 0], after_z),
        )

    def send_over(c):
        @pl.when(last)
        def _():
            c[0].start()
            if more:
                c[1].start()

        @pl.when(first)
        def _():
            c[2].start()
            if more:
                c[3].start()

    def send_inside(c):
        pl.when(not_last)(c[0].start)
        pl.when(not_first)(c[1].start)

    def coef_copy(role, source, target, device):
        return pltpu.make_async_remote_copy(
            src_ref=source, dst_ref=target,
            send_sem=coef_send.at[role], recv_sem=coef_recv.at[role],
            device_id=device, device_id_type=MESH,
        )

    tall = rows + 8
    coef_y = (
        coef_copy(4, yc_out.at[0], yc_in.at[1], before_y),
        coef_copy(5, yc_out.at[1], yc_in.at[0], after_y),
    )

    def coef_piece(role, piece, start, size, side, device):
        return coef_copy(
            role, xc_out.at[piece, pl.ds(start, size)],
            xc_in.at[side, pl.ds(piece * tall + start, size)], device,
        )

    lines = ((floor, ceiling), (rows - ceiling, rows - floor))
    coef_x = () if aligned else (
        coef_piece(0, 0, floor, rows - floor + 8, 0, up[0]),
        coef_piece(1, 1, 0, ceiling + 8, 0, up[1]),
        coef_piece(2, 0, rows - ceiling, ceiling + 8, 1, down[0]),
        coef_piece(3, 1, 0, rows - floor + 8, 1, down[1]),
    )

    lane = lax.broadcasted_iota(jnp.int32, (8, lanes), 1)
    row = lax.broadcasted_iota(jnp.int32, (8, lanes), 0)
    even = lane % 2 == 0

    def turn(value, amount):
        amount = amount % lanes
        return pltpu.roll(value, amount, 1) if amount else value

    def spot_of(block, x):
        return span * (block % per) + 2 * x

    def pack(t, p, cells, fresh):
        packed = [
            jnp.zeros((8, lanes), jnp.float32) if fresh else z_out[t, group]
            for group in range(groups)
        ]
        for block, x in cells:
            spot = spot_of(block, x)
            moved = turn(field[p, x, pl.ds(PAD + 8 * block, 8)], spot + 1)
            group = block // per
            packed[group] = jnp.where(
                (lane == spot) | (lane == spot + 1), moved, packed[group]
            )
        for group, value in enumerate(packed):
            z_out[t, group] = value

    every = [(block, x) for block in range(blocks) for x in range(nx)]
    inner = [(b, x) for b, x in every if 0 < b < blocks - 1 and 0 < x < nx - 1]
    outer = [cell for cell in every if cell not in inner]

    loads = (
        pltpu.make_async_copy(conc, field.at[0, :, body_rows], load_sem.at[0]),
        pltpu.make_async_copy(diff, d_buf, load_sem.at[1]),
        pltpu.make_async_copy(speed, v_buf, load_sem.at[2]),
        pltpu.make_async_copy(signs, s_buf, load_sem.at[3]),
    )
    for load in loads:
        load.start()

    nil = jnp.zeros((8, lanes), jnp.float32)
    for p in range(2):
        for x in range(nx):
            field[p, x, pl.ds(0, PAD)] = nil
            field[p, x, pl.ds(PAD + rows, PAD)] = nil
    if not aligned:
        for side in range(2):
            for p in range(2):
                halo[p, side, pl.ds(0, 8)] = nil
                halo[p, side, pl.ds(8 + rows, 8)] = nil
            for block in range(2 * blocks):
                window[side, pl.ds(8 * block, 8)] = nil
            for block in range(2 * tall // 8):
                xc_in[side, pl.ds(8 * block, 8)] = nil

    barrier = pltpu.get_barrier_semaphore()

    def greet(device):
        pl.semaphore_signal(barrier, inc=1, device_id=device, device_id_type=MESH)

    for device in (up[0], down[0], before_y, after_y, before_z, after_z):
        greet(device)
    if more:
        pl.when(last)(lambda: greet(up[1]))
        pl.when(first)(lambda: greet(down[1]))
    loads[0].wait()
    for x in range(nx):
        for side, edge in enumerate((PAD, PAD + rows - 1)):
            line = field[0, x, pl.ds(edge, 1)]
            y_out[0, side, pl.ds(x, 1)] = line
            own_y[0, side, pl.ds(x, 1)] = line
    pack(0, 0, every, True)
    for load in loads[1:]:
        load.wait()

    def weigh(x, carry):
        d = time_step * d_buf[x]
        centre = 1.0 - 6.0 * d
        plane_lane = lax.broadcasted_iota(jnp.int32, (rows, lanes), 1)
        for axis in range(3):
            v = time_step * v_buf[axis, x]
            forward = s_buf[axis, x] > 0
            below = jnp.where(forward, v, 0.0)
            above = v - below
            centre = centre - below + above
            minus, plus = d + below, d - above
            if axis == 2:
                low_end, high_end = plane_lane == 0, plane_lane == lanes - 1
                coef[7, x] = jnp.where(low_end, minus, jnp.where(high_end, plus, 0.0))
                minus = jnp.where(low_end, 0.0, minus)
                plus = jnp.where(high_end, 0.0, plus)
            coef[1 + 2 * axis, x] = minus
            coef[2 + 2 * axis, x] = plus
        coef[0, x] = centre
        return carry

    lax.fori_loop(0, nx, weigh, 0)

    for x in range(nx):
        yc_out[0, pl.ds(x, 1)] = coef[3, x, pl.ds(0, 1)]
        yc_out[1, pl.ds(x, 1)] = coef[4, x, pl.ds(rows - 1, 1)]
    if not aligned:
        for block in range(blocks):
            value = jnp.where(
                first, coef[1, 0, pl.ds(8 * block, 8)], coef[2, nx - 1, pl.ds(8 * block, 8)]
            )
            xc_out[0, pl.ds(8 + 8 * block, 8)] = value
            xc_out[1, pl.ds(8 * block, 8)] = value
        top_line = jnp.where(first, coef[4, 0, pl.ds(rows - 1, 1)], coef[4, nx - 1, pl.ds(rows - 1, 1)])
        low_line = jnp.where(first, coef[3, 0, pl.ds(0, 1)], coef[3, nx - 1, pl.ds(0, 1)])
        for here, (start, end) in zip((last, first), lines):
            @pl.when(here)
            def _(start=start, end=end):
                xc_out[0, pl.ds(start, 8)] = jnp.broadcast_to(top_line, (8, lanes))
                xc_out[1, pl.ds(end, 8)] = jnp.broadcast_to(low_line, (8, lanes))

    pl.semaphore_wait(barrier, 6 + (jnp.where(first | last, 1, 0) if more else 0))
    send_over(field_over(0, 0))
    send_inside(inside_planes(0, 0))
    for copy in edges(0):
        copy.start()
    if not aligned:
        send_over(coef_x)
    for copy in coef_y:
        copy.start()

    residue = 0 if aligned else lax.rem(shear[0], rows)
    starts = (0, 0) if aligned else (
        jnp.where(first, residue, 0), jnp.where(last, rows - residue, 0)
    )

    def step(t, carry):
        p = lax.rem(t, 2)
        q = 1 - p
        after = t + 1
        goes_on = after < STEPS

        for x in range(nx):
            for block in range(blocks):
                start = PAD + 8 * block
                rows8 = pl.ds(8 * block, 8)
                here = field[p, x, pl.ds(start, 8)]
                total = (
                    coef[0, x, rows8] * here
                    + coef[3, x, rows8] * field[p, x, pl.ds(start - 1, 8)]
                ) + (
                    coef[4, x, rows8] * field[p, x, pl.ds(start + 1, 8)]
                    + (coef[5, x, rows8] * turn(here, 1) + coef[6, x, rows8] * turn(here, -1))
                )
                if x > 0:
                    total = total + coef[1, x, rows8] * field[p, x - 1, pl.ds(start, 8)]
                if x < nx - 1:
                    total = total + coef[2, x, rows8] * field[p, x + 1, pl.ds(start, 8)]
                if x in ends:
                    part[after, ends.index(x), rows8] = total
                else:
                    field[q, x, pl.ds(start, 8)] = total

        e = edges(t)
        e[2].wait_recv()
        e[3].wait_recv()
        sides = [
            jnp.where(even, z_in[t, 0, group], turn(z_in[t, 1, group], -2))
            for group in range(groups)
        ]

        def add_side(block, x):
            rows8 = pl.ds(8 * block, 8)
            more_z = coef[7, x, rows8] * turn(sides[block // per], -spot_of(block, x))
            if x in ends:
                s = ends.index(x)
                part[after, s, rows8] = part[after, s, rows8] + more_z
            else:
                place = pl.ds(PAD + 8 * block, 8)
                field[q, x, place] = field[q, x, place] + more_z

        for x in ends:
            for block in range(blocks):
                add_side(block, x)
        if not aligned:
            pl.when(goes_on)(lambda: send_over(part_over(after)))
        for x in range(1, nx - 1):
            for block in range(blocks):
                add_side(block, x)
        pack(after, q, inner, True)
        for x in range(1, nx - 1):
            for side, edge in enumerate((PAD, PAD + rows - 1)):
                y_out[after, side, pl.ds(x, 1)] = field[q, x, pl.ds(edge, 1)]

        over, inside = field_over(t, p), inside_planes(t, p)

        @pl.when(first)
        def _():
            over[0].wait_recv()
            if more:
                over[1].wait_recv()

        @pl.when(last)
        def _():
            over[2].wait_recv()
            if more:
                over[3].wait_recv()

        pl.when(not_first)(inside[0].wait_recv)
        pl.when(not_last)(inside[1].wait_recv)

        def received(side, block):
            if aligned:
                return x_in[t, side, pl.ds(8 * block, 8)]
            return window[side, pl.ds(starts[side] + 8 * block, 8)]

        def unpack(side, begin, end):
            for r in range(begin, end, 8):
                window[side, pl.ds(r, 8)] = x_in[t, side, pl.ds(r, 8)]

        if not aligned:
            pl.when(first)(lambda: unpack(0, floor, rows + ceiling))
            pl.when(not_first)(lambda: unpack(0, 0, rows))
            pl.when(last)(lambda: unpack(1, rows - ceiling, 2 * rows - floor))
            pl.when(not_last)(lambda: unpack(1, 0, rows))

        if not aligned:
            @pl.when(t == 0)
            def _():
                for side in range(2):
                    for block in range(blocks):
                        halo[0, side, pl.ds(8 + 8 * block, 8)] = received(side, block)

            @pl.when(t == 1)
            def _():
                @pl.when(first)
                def _():
                    coef_x[0].wait_recv()
                    coef_x[1].wait_recv()

                @pl.when(last)
                def _():
                    coef_x[2].wait_recv()
                    coef_x[3].wait_recv()

            @pl.when(t > 0)
            def _():
                for side in range(2):
                    top_line = xc_in[side, pl.ds(lines[side][0], 8)]
                    low_line = xc_in[side, pl.ds(tall + lines[side][1], 8)]
                    seam = rows - 1 - starts[side]
                    for block in range(blocks):
                        base = 8 + 8 * block
                        value = received(side, block) + (
                            xc_in[side, pl.ds(starts[side] + base, 8)]
                            * field[q, ends[side], pl.ds(PAD + 8 * block, 8)]
                        )
                        value = value + jnp.where(
                            row == seam - 8 * block,
                            top_line * halo[q, side, pl.ds(base + 1, 8)], 0.0,
                        )
                        value = value + jnp.where(
                            row == seam + 1 - 8 * block,
                            low_line * halo[q, side, pl.ds(base - 1, 8)], 0.0,
                        )
                        halo[p, side, pl.ds(base, 8)] = value

        for side in range(2):
            x = ends[side]
            for block in range(blocks):
                rows8 = pl.ds(8 * block, 8)
                beyond = received(side, block) if aligned else halo[p, side, pl.ds(8 + 8 * block, 8)]
                field[q, x, pl.ds(PAD + 8 * block, 8)] = (
                    part[after, side, rows8] + coef[1 + side, x, rows8] * beyond
                )
            y_out[after, 0, pl.ds(x, 1)] = field[q, x, pl.ds(PAD, 1)]
            y_out[after, 1, pl.ds(x, 1)] = field[q, x, pl.ds(PAD + rows - 1, 1)]
        later = edges(after)

        @pl.when(goes_on)
        def _():
            later[0].start()
            later[1].start()

        e[0].wait_recv()
        e[1].wait_recv()

        @pl.when(t == 1)
        def _():
            for copy in coef_y:
                copy.wait_recv()

        @pl.when(t == 0)
        def _():
            for side in range(2):
                own_y[1, side] = y_out[after, side] + yc_out[side] * y_in[t, side]

        @pl.when(t > 0)
        def _():
            for side in range(2):
                beyond = y_in[t, side] + yc_in[side] * own_y[q, side]
                own_y[q, side] = y_out[after, side] + yc_out[side] * beyond

        for side, edge in enumerate((PAD, PAD + rows - 1)):
            for x in (0, nx - 1, *range(1, nx - 1)):
                field[q, x, pl.ds(edge, 1)] = own_y[q, side, pl.ds(x, 1)]

        @pl.when(last)
        def _():
            over[0].wait_send()
            if more:
                over[1].wait_send()

        @pl.when(first)
        def _():
            over[2].wait_send()
            if more:
                over[3].wait_send()

        pl.when(not_last)(inside[0].wait_send)
        pl.when(not_first)(inside[1].wait_send)
        for copy in e:
            copy.wait_send()

        @pl.when(goes_on)
        def _():
            send_inside(inside_planes(after, q))
            if aligned:
                send_over(field_over(after, q))

        pack(after, q, outer, False)

        @pl.when(goes_on)
        def _():
            later[2].start()
            later[3].start()

        return carry

    lax.fori_loop(0, STEPS, step, 0)
    store = pltpu.make_async_copy(field.at[STEPS % 2, :, body_rows], out, load_sem.at[0])
    store.start()
    for copy in coef_y:
        copy.wait_send()
    if not aligned:
        @pl.when(last)
        def _():
            coef_x[0].wait_send()
            coef_x[1].wait_send()

        @pl.when(first)
        def _():
            coef_x[2].wait_send()
            coef_x[3].wait_send()
    store.wait()


def run(hops, aligned, floor, width, index, counts, shear, conc, speed, signs, diff):
    nx, rows, lanes = conc.shape
    f32 = jnp.float32
    groups = (rows // 8) // (lanes // (2 * nx))
    anywhere = pl.BlockSpec(memory_space=pl.ANY)
    return pl.pallas_call(
        functools.partial(kernel, hops, aligned, floor, width, *counts),
        name=f"slide{index}",
        out_shape=jax.ShapeDtypeStruct(conc.shape, f32),
        in_specs=[pl.BlockSpec(memory_space=pltpu.SMEM)] + [anywhere] * 4,
        out_specs=anywhere,
        scratch_shapes=[
            pltpu.VMEM((2, nx, rows + 2 * PAD, lanes), f32),
            pltpu.VMEM((8, nx, rows, lanes), f32),
            pltpu.VMEM((3, nx, rows, lanes), f32),
            pltpu.VMEM((3, nx, rows, lanes), jnp.int32),
            pltpu.VMEM((nx, rows, lanes), f32),
            pltpu.VMEM((STEPS + 1, 2, rows, lanes), f32),
            pltpu.VMEM((STEPS, 2, 2 * rows, lanes), f32),
            pltpu.VMEM((2, 2 * rows, lanes), f32),
            pltpu.VMEM((2, 2, rows + 16, lanes), f32),
            pltpu.VMEM((2, rows + 8, lanes), f32),
            pltpu.VMEM((2, 2 * rows + 16, lanes), f32),
            pltpu.VMEM((STEPS + 1, 2, nx, lanes), f32),
            pltpu.VMEM((STEPS, 2, nx, lanes), f32),
            pltpu.VMEM((2, nx, lanes), f32),
            pltpu.VMEM((2, nx, lanes), f32),
            pltpu.VMEM((2, 2, nx, lanes), f32),
            pltpu.VMEM((STEPS + 1, groups, 8, lanes), f32),
            pltpu.VMEM((STEPS, 2, groups, 8, lanes), f32),
            pltpu.SemaphoreType.DMA((4,)),
            pltpu.SemaphoreType.DMA((TURNS, 8)),
            pltpu.SemaphoreType.DMA((TURNS, 8)),
            pltpu.SemaphoreType.DMA((6,)),
            pltpu.SemaphoreType.DMA((6,)),
        ],
        compiler_params=pltpu.CompilerParams(
            collective_id=index, has_side_effects=True
        ),
    )(shear, conc, speed, signs, diff)


def body(concentration, speed, signs, diffusivity, shear):
    counts = tuple(lax.axis_size(name) for name in ("gx", "gy", "gz"))
    rows = concentration.shape[1]
    width = rows // BUCKETS
    kinds = [(True, 0, 0)] + [(False, width * bucket, width) for bucket in range(BUCKETS)]
    branches = [
        functools.partial(run, hops, *kind, hops * len(kinds) + number, counts)
        for hops in range(counts[1]) for number, kind in enumerate(kinds)
    ]
    hops, residue = lax.div(shear[0], rows), lax.rem(shear[0], rows)
    number = jnp.where(residue == 0, 0, 1 + lax.div(residue, width))
    return lax.switch(
        len(kinds) * hops + number, branches, shear, concentration, speed, signs, diffusivity
    )


def solution(mesh):
    placed = (
        P("gx", "gy", "gz"),
        P(None, "gx", "gy", "gz"),
        P(None, "gx", "gy", "gz"),
        P("gx", "gy", "gz"),
        P(),
    )
    return jax.shard_map(
        body, mesh=mesh, in_specs=placed, out_specs=P("gx", "gy", "gz"), check_vma=False
    )
```

```python
import functools

import jax
import jax.numpy as jnp
from jax import lax
from jax.experimental import pallas as pl
from jax.experimental.pallas import tpu as pltpu
from jax.sharding import PartitionSpec as P

STEPS = 8
time_step = 0.25
PAD = 8
TURNS = 4
MESH = pl.DeviceIdType.MESH


def kernel(
    hops, aligned, floor, width, count_x, count_y, count_z,
    shear, conc, speed, signs, diff, out,
    field, coef, v_buf, s_buf, d_buf, part, x_in, window, halo, xc_out, xc_in,
    y_out, y_in, yc_out, yc_in, own_y, z_out, z_in,
    load_sem, send_sem, recv_sem, coef_send, coef_recv,
):
    nx, rows, lanes = conc.shape
    blocks = rows // 8
    span = 2 * nx
    per = lanes // span
    groups = blocks // per
    ends = (0, nx - 1)
    gx, gy, gz = (lax.axis_index(name) for name in ("gx", "gy", "gz"))
    first, last = gx == 0, gx == count_x - 1
    not_first, not_last = gx != 0, gx != count_x - 1
    body_rows = pl.ds(PAD, rows)

    def at(x, y):
        return {"gx": x, "gy": lax.rem(y + 2 * count_y, count_y)}

    more = 0 if aligned else 1
    up = (
        at(jnp.where(last, 0, gx + 1), gy - jnp.where(last, hops, 0)),
        at(0, gy - hops - 1),
    )
    down = (
        at(jnp.where(first, count_x - 1, gx - 1), gy + jnp.where(first, hops + more, 0)),
        at(count_x - 1, gy + hops),
    )
    before_y, after_y = at(gx, gy - 1), at(gx, gy + 1)
    before_z = {"gz": lax.rem(gz + count_z - 1, count_z)}
    after_z = {"gz": lax.rem(gz + 1, count_z)}

    def remote(t, role, source, target, device):
        return pltpu.make_async_remote_copy(
            src_ref=source, dst_ref=target,
            send_sem=send_sem.at[t % TURNS, role], recv_sem=recv_sem.at[t % TURNS, role],
            device_id=device, device_id_type=MESH,
        )

    ceiling = floor + width

    def over_planes(t, top, bottom):
        if aligned:
            return (
                remote(t, 0, top(0, rows), x_in.at[t, 0, pl.ds(0, rows)], up[0]), None,
                remote(t, 2, bottom(0, rows), x_in.at[t, 1, pl.ds(0, rows)], down[0]), None,
            )
        far, near = rows - ceiling, rows - floor
        return (
            remote(t, 0, top(floor, near), x_in.at[t, 0, pl.ds(floor, near)], up[0]),
            remote(t, 1, top(0, ceiling), x_in.at[t, 0, pl.ds(rows, ceiling)], up[1]),
            remote(t, 2, bottom(far, ceiling), x_in.at[t, 1, pl.ds(far, ceiling)], down[0]),
            remote(t, 3, bottom(0, near), x_in.at[t, 1, pl.ds(rows, near)], down[1]),
        )

    def field_over(t, p):
        return over_planes(
            t,
            lambda a, n: field.at[p, nx - 1, pl.ds(PAD + a, n)],
            lambda a, n: field.at[p, 0, pl.ds(PAD + a, n)],
        )

    def part_over(t):
        return over_planes(
            t, lambda a, n: part.at[t, 1, pl.ds(a, n)], lambda a, n: part.at[t, 0, pl.ds(a, n)]
        )

    def inside_planes(t, p):
        return (
            remote(t, 0, field.at[p, nx - 1, body_rows], x_in.at[t, 0, pl.ds(0, rows)], up[0]),
            remote(t, 2, field.at[p, 0, body_rows], x_in.at[t, 1, pl.ds(0, rows)], down[0]),
        )

    def edges(t):
        return (
            remote(t, 4, y_out.at[t, 0], y_in.at[t, 1], before_y),
            remote(t, 5, y_out.at[t, 1], y_in.at[t, 0], after_y),
            remote(t, 6, z_out.at[t], z_in.at[t, 1], before_z),
            remote(t, 7, z_out.at[t], z_in.at[t, 0], after_z),
        )

    def send_over(c):
        @pl.when(last)
        def _():
            c[0].start()
            if more:
                c[1].start()

        @pl.when(first)
        def _():
            c[2].start()
            if more:
                c[3].start()

    def send_inside(c):
        pl.when(not_last)(c[0].start)
        pl.when(not_first)(c[1].start)

    def coef_copy(role, source, target, device):
        return pltpu.make_async_remote_copy(
            src_ref=source, dst_ref=target,
            send_sem=coef_send.at[role], recv_sem=coef_recv.at[role],
            device_id=device, device_id_type=MESH,
        )

    tall = rows + 8
    coef_y = (
        coef_copy(4, yc_out.at[0], yc_in.at[1], before_y),
        coef_copy(5, yc_out.at[1], yc_in.at[0], after_y),
    )

    def coef_piece(role, piece, start, size, side, device):
        return coef_copy(
            role, xc_out.at[piece, pl.ds(start, size)],
            xc_in.at[side, pl.ds(piece * tall + start, size)], device,
        )

    lines = ((floor, ceiling), (rows - ceiling, rows - floor))
    coef_x = () if aligned else (
        coef_piece(0, 0, floor, rows - floor + 8, 0, up[0]),
        coef_piece(1, 1, 0, ceiling + 8, 0, up[1]),
        coef_piece(2, 0, rows - ceiling, ceiling + 8, 1, down[0]),
        coef_piece(3, 1, 0, rows - floor + 8, 1, down[1]),
    )

    lane = lax.broadcasted_iota(jnp.int32, (8, lanes), 1)
    row = lax.broadcasted_iota(jnp.int32, (8, lanes), 0)
    even = lane % 2 == 0

    def turn(value, amount):
        amount = amount % lanes
        return pltpu.roll(value, amount, 1) if amount else value

    def spot_of(block, x):
        return span * (block % per) + 2 * x

    def pack(t, p, cells, fresh):
        packed = [
            jnp.zeros((8, lanes), jnp.float32) if fresh else z_out[t, group]
            for group in range(groups)
        ]
        for block, x in cells:
            spot = spot_of(block, x)
            moved = turn(field[p, x, pl.ds(PAD + 8 * block, 8)], spot + 1)
            group = block // per
            packed[group] = jnp.where(
                (lane == spot) | (lane == spot + 1), moved, packed[group]
            )
        for group, value in enumerate(packed):
            z_out[t, group] = value

    every = [(block, x) for block in range(blocks) for x in range(nx)]
    inner = [(b, x) for b, x in every if 0 < b < blocks - 1 and 0 < x < nx - 1]
    outer = [cell for cell in every if cell not in inner]

    loads = (
        pltpu.make_async_copy(conc, field.at[0, :, body_rows], load_sem.at[0]),
        pltpu.make_async_copy(diff, d_buf, load_sem.at[1]),
        pltpu.make_async_copy(speed, v_buf, load_sem.at[2]),
        pltpu.make_async_copy(signs, s_buf, load_sem.at[3]),
    )
    for load in loads:
        load.start()

    nil = jnp.zeros((8, lanes), jnp.float32)
    if not aligned:
        for side in range(2):
            for block in range(2 * tall // 8):
                xc_in[side, pl.ds(8 * block, 8)] = nil

    barrier = pltpu.get_barrier_semaphore()

    def greet(device):
        pl.semaphore_signal(barrier, inc=1, device_id=device, device_id_type=MESH)

    if more:
        pl.when(last)(lambda: greet(up[1]))
        pl.when(first)(lambda: greet(down[1]))
    for device in (up[0], down[0], before_y, after_y, before_z, after_z):
        greet(device)
    for p in range(2):
        for x in range(nx):
            field[p, x, pl.ds(0, PAD)] = nil
            field[p, x, pl.ds(PAD + rows, PAD)] = nil
    if not aligned:
        for side in range(2):
            for p in range(2):
                halo[p, side, pl.ds(0, 8)] = nil
                halo[p, side, pl.ds(8 + rows, 8)] = nil
            for block in range(2 * blocks):
                window[side, pl.ds(8 * block, 8)] = nil

    loads[0].wait()
    for x in range(nx):
        for side, edge in enumerate((PAD, PAD + rows - 1)):
            line = field[0, x, pl.ds(edge, 1)]
            y_out[0, side, pl.ds(x, 1)] = line
            own_y[0, side, pl.ds(x, 1)] = line
    pack(0, 0, every, True)
    for load in loads[1:]:
        load.wait()

    def weigh(x, carry):
        d = time_step * d_buf[x]
        centre = 1.0 - 6.0 * d
        plane_lane = lax.broadcasted_iota(jnp.int32, (rows, lanes), 1)
        for axis in range(3):
            v = time_step * v_buf[axis, x]
            forward = s_buf[axis, x] > 0
            below = jnp.where(forward, v, 0.0)
            above = v - below
            centre = centre - below + above
            minus, plus = d + below, d - above
            if axis == 2:
                low_end, high_end = plane_lane == 0, plane_lane == lanes - 1
                coef[7, x] = jnp.where(low_end, minus, jnp.where(high_end, plus, 0.0))
                minus = jnp.where(low_end, 0.0, minus)
                plus = jnp.where(high_end, 0.0, plus)
            coef[1 + 2 * axis, x] = minus
            coef[2 + 2 * axis, x] = plus
        coef[0, x] = centre
        return carry

    lax.fori_loop(0, nx, weigh, 0)

    for x in range(nx):
        yc_out[0, pl.ds(x, 1)] = coef[3, x, pl.ds(0, 1)]
        yc_out[1, pl.ds(x, 1)] = coef[4, x, pl.ds(rows - 1, 1)]
    if not aligned:
        for block in range(blocks):
            value = jnp.where(
                first, coef[1, 0, pl.ds(8 * block, 8)], coef[2, nx - 1, pl.ds(8 * block, 8)]
            )
            xc_out[0, pl.ds(8 + 8 * block, 8)] = value
            xc_out[1, pl.ds(8 * block, 8)] = value
        top_line = jnp.where(first, coef[4, 0, pl.ds(rows - 1, 1)], coef[4, nx - 1, pl.ds(rows - 1, 1)])
        low_line = jnp.where(first, coef[3, 0, pl.ds(0, 1)], coef[3, nx - 1, pl.ds(0, 1)])
        for here, (start, end) in zip((last, first), lines):
            @pl.when(here)
            def _(start=start, end=end):
                xc_out[0, pl.ds(start, 8)] = jnp.broadcast_to(top_line, (8, lanes))
                xc_out[1, pl.ds(end, 8)] = jnp.broadcast_to(low_line, (8, lanes))

    pl.semaphore_wait(barrier, 6 + (jnp.where(first | last, 1, 0) if more else 0))
    send_over(field_over(0, 0))
    send_inside(inside_planes(0, 0))
    for copy in edges(0):
        copy.start()
    if not aligned:
        send_over(coef_x)
    for copy in coef_y:
        copy.start()

    residue = 0 if aligned else lax.rem(shear[0], rows)
    starts = (0, 0) if aligned else (
        jnp.where(first, residue, 0), jnp.where(last, rows - residue, 0)
    )

    def step(t, carry):
        p = lax.rem(t, 2)
        q = 1 - p
        after = t + 1
        goes_on = after < STEPS

        for x in range(nx):
            for block in range(blocks):
                start = PAD + 8 * block
                rows8 = pl.ds(8 * block, 8)
                here = field[p, x, pl.ds(start, 8)]
                total = (
                    coef[0, x, rows8] * here
                    + coef[3, x, rows8] * field[p, x, pl.ds(start - 1, 8)]
                ) + (
                    coef[4, x, rows8] * field[p, x, pl.ds(start + 1, 8)]
                    + (coef[5, x, rows8] * turn(here, 1) + coef[6, x, rows8] * turn(here, -1))
                )
                if x > 0:
                    total = total + coef[1, x, rows8] * field[p, x - 1, pl.ds(start, 8)]
                if x < nx - 1:
                    total = total + coef[2, x, rows8] * field[p, x + 1, pl.ds(start, 8)]
                if x in ends:
                    part[after, ends.index(x), rows8] = total
                else:
                    field[q, x, pl.ds(start, 8)] = total

        e = edges(t)
        e[2].wait_recv()
        e[3].wait_recv()
        sides = [
            jnp.where(even, z_in[t, 0, group], turn(z_in[t, 1, group], -2))
            for group in range(groups)
        ]

        def add_side(block, x):
            rows8 = pl.ds(8 * block, 8)
            more_z = coef[7, x, rows8] * turn(sides[block // per], -spot_of(block, x))
            if x in ends:
                s = ends.index(x)
                part[after, s, rows8] = part[after, s, rows8] + more_z
            else:
                place = pl.ds(PAD + 8 * block, 8)
                field[q, x, place] = field[q, x, place] + more_z

        for x in ends:
            for block in range(blocks):
                add_side(block, x)
        if not aligned:
            pl.when(goes_on)(lambda: send_over(part_over(after)))
        for x in range(1, nx - 1):
            for block in range(blocks):
                add_side(block, x)
        pack(after, q, inner, True)
        for x in range(1, nx - 1):
            for side, edge in enumerate((PAD, PAD + rows - 1)):
                y_out[after, side, pl.ds(x, 1)] = field[q, x, pl.ds(edge, 1)]

        over, inside = field_over(t, p), inside_planes(t, p)

        @pl.when(first)
        def _():
            over[0].wait_recv()
            if more:
                over[1].wait_recv()

        @pl.when(last)
        def _():
            over[2].wait_recv()
            if more:
                over[3].wait_recv()

        pl.when(not_first)(inside[0].wait_recv)
        pl.when(not_last)(inside[1].wait_recv)

        def received(side, block):
            if aligned:
                return x_in[t, side, pl.ds(8 * block, 8)]
            return window[side, pl.ds(starts[side] + 8 * block, 8)]

        def unpack(side, begin, end):
            for r in range(begin, end, 8):
                window[side, pl.ds(r, 8)] = x_in[t, side, pl.ds(r, 8)]

        if not aligned:
            pl.when(first)(lambda: unpack(0, floor, rows + ceiling))
            pl.when(not_first)(lambda: unpack(0, 0, rows))
            pl.when(last)(lambda: unpack(1, rows - ceiling, 2 * rows - floor))
            pl.when(not_last)(lambda: unpack(1, 0, rows))

        if not aligned:
            @pl.when(t == 0)
            def _():
                for side in range(2):
                    for block in range(blocks):
                        halo[0, side, pl.ds(8 + 8 * block, 8)] = received(side, block)

            @pl.when(t == 1)
            def _():
                @pl.when(first)
                def _():
                    coef_x[0].wait_recv()
                    coef_x[1].wait_recv()

                @pl.when(last)
                def _():
                    coef_x[2].wait_recv()
                    coef_x[3].wait_recv()

            @pl.when(t > 0)
            def _():
                for side in range(2):
                    top_line = xc_in[side, pl.ds(lines[side][0], 8)]
                    low_line = xc_in[side, pl.ds(tall + lines[side][1], 8)]
                    seam = rows - 1 - starts[side]
                    for block in range(blocks):
                        base = 8 + 8 * block
                        value = received(side, block) + (
                            xc_in[side, pl.ds(starts[side] + base, 8)]
                            * field[q, ends[side], pl.ds(PAD + 8 * block, 8)]
                        )
                        value = value + jnp.where(
                            row == seam - 8 * block,
                            top_line * halo[q, side, pl.ds(base + 1, 8)], 0.0,
                        )
                        value = value + jnp.where(
                            row == seam + 1 - 8 * block,
                            low_line * halo[q, side, pl.ds(base - 1, 8)], 0.0,
                        )
                        halo[p, side, pl.ds(base, 8)] = value

        for side in range(2):
            x = ends[side]
            for block in range(blocks):
                rows8 = pl.ds(8 * block, 8)
                beyond = received(side, block) if aligned else halo[p, side, pl.ds(8 + 8 * block, 8)]
                field[q, x, pl.ds(PAD + 8 * block, 8)] = (
                    part[after, side, rows8] + coef[1 + side, x, rows8] * beyond
                )
            y_out[after, 0, pl.ds(x, 1)] = field[q, x, pl.ds(PAD, 1)]
            y_out[after, 1, pl.ds(x, 1)] = field[q, x, pl.ds(PAD + rows - 1, 1)]
        later = edges(after)

        @pl.when(goes_on)
        def _():
            later[0].start()
            later[1].start()

        e[0].wait_recv()
        e[1].wait_recv()

        @pl.when(t == 1)
        def _():
            for copy in coef_y:
                copy.wait_recv()

        @pl.when(t == 0)
        def _():
            for side in range(2):
                own_y[1, side] = y_out[after, side] + yc_out[side] * y_in[t, side]

        @pl.when(t > 0)
        def _():
            for side in range(2):
                beyond = y_in[t, side] + yc_in[side] * own_y[q, side]
                own_y[q, side] = y_out[after, side] + yc_out[side] * beyond

        def put_rows(xs):
            for side, edge in enumerate((PAD, PAD + rows - 1)):
                for x in xs:
                    field[q, x, pl.ds(edge, 1)] = own_y[q, side, pl.ds(x, 1)]

        put_rows(ends)

        @pl.when(goes_on)
        def _():
            send_inside(inside_planes(after, q))
            if aligned:
                send_over(field_over(after, q))

        put_rows(range(1, nx - 1))
        pack(after, q, outer, False)

        @pl.when(goes_on)
        def _():
            later[2].start()
            later[3].start()

        @pl.when(last)
        def _():
            over[0].wait_send()
            if more:
                over[1].wait_send()

        @pl.when(first)
        def _():
            over[2].wait_send()
            if more:
                over[3].wait_send()

        pl.when(not_last)(inside[0].wait_send)
        pl.when(not_first)(inside[1].wait_send)
        for copy in e:
            copy.wait_send()

        return carry

    lax.fori_loop(0, STEPS, step, 0)
    store = pltpu.make_async_copy(field.at[STEPS % 2, :, body_rows], out, load_sem.at[0])
    store.start()
    for copy in coef_y:
        copy.wait_send()
    if not aligned:
        @pl.when(last)
        def _():
            coef_x[0].wait_send()
            coef_x[1].wait_send()

        @pl.when(first)
        def _():
            coef_x[2].wait_send()
            coef_x[3].wait_send()
    store.wait()


def run(hops, aligned, floor, width, index, counts, shear, conc, speed, signs, diff):
    nx, rows, lanes = conc.shape
    f32 = jnp.float32
    groups = (rows // 8) // (lanes // (2 * nx))
    anywhere = pl.BlockSpec(memory_space=pl.ANY)
    return pl.pallas_call(
        functools.partial(kernel, hops, aligned, floor, width, *counts),
        name=f"slide{index}",
        out_shape=jax.ShapeDtypeStruct(conc.shape, f32),
        in_specs=[pl.BlockSpec(memory_space=pltpu.SMEM)] + [anywhere] * 4,
        out_specs=anywhere,
        scratch_shapes=[
            pltpu.VMEM((2, nx, rows + 2 * PAD, lanes), f32),
            pltpu.VMEM((8, nx, rows, lanes), f32),
            pltpu.VMEM((3, nx, rows, lanes), f32),
            pltpu.VMEM((3, nx, rows, lanes), jnp.int32),
            pltpu.VMEM((nx, rows, lanes), f32),
            pltpu.VMEM((STEPS + 1, 2, rows, lanes), f32),
            pltpu.VMEM((STEPS, 2, 2 * rows, lanes), f32),
            pltpu.VMEM((2, 2 * rows, lanes), f32),
            pltpu.VMEM((2, 2, rows + 16, lanes), f32),
            pltpu.VMEM((2, rows + 8, lanes), f32),
            pltpu.VMEM((2, 2 * rows + 16, lanes), f32),
            pltpu.VMEM((STEPS + 1, 2, nx, lanes), f32),
            pltpu.VMEM((STEPS, 2, nx, lanes), f32),
            pltpu.VMEM((2, nx, lanes), f32),
            pltpu.VMEM((2, nx, lanes), f32),
            pltpu.VMEM((2, 2, nx, lanes), f32),
            pltpu.VMEM((STEPS + 1, groups, 8, lanes), f32),
            pltpu.VMEM((STEPS, 2, groups, 8, lanes), f32),
            pltpu.SemaphoreType.DMA((4,)),
            pltpu.SemaphoreType.DMA((TURNS, 8)),
            pltpu.SemaphoreType.DMA((TURNS, 8)),
            pltpu.SemaphoreType.DMA((6,)),
            pltpu.SemaphoreType.DMA((6,)),
        ],
        compiler_params=pltpu.CompilerParams(
            collective_id=index, has_side_effects=True
        ),
    )(shear, conc, speed, signs, diff)


def body(concentration, speed, signs, diffusivity, shear):
    counts = tuple(lax.axis_size(name) for name in ("gx", "gy", "gz"))
    rows = concentration.shape[1]
    kinds, before = [], []
    for hops in range(counts[1]):
        before.append(len(kinds))
        width = rows // (4 if 0 < hops < counts[1] - 1 else 2)
        kinds.append((hops, True, 0, 0))
        kinds.extend((hops, False, floor, width) for floor in range(0, rows, width))
    branches = [
        functools.partial(run, *kind, number, counts) for number, kind in enumerate(kinds)
    ]
    hops, residue = lax.div(shear[0], rows), lax.rem(shear[0], rows)
    finer = (hops > 0) & (hops < counts[1] - 1)
    part = jnp.where(finer, lax.div(residue, rows // 4), lax.div(residue, rows // 2))
    base = sum(jnp.where(hops == h, first, 0) for h, first in enumerate(before))
    return lax.switch(
        base + jnp.where(residue == 0, 0, 1 + part),
        branches, shear, concentration, speed, signs, diffusivity,
    )


def solution(mesh):
    placed = (
        P("gx", "gy", "gz"),
        P(None, "gx", "gy", "gz"),
        P(None, "gx", "gy", "gz"),
        P("gx", "gy", "gz"),
        P(),
    )
    return jax.shard_map(
        body, mesh=mesh, in_specs=placed, out_specs=P("gx", "gy", "gz"), check_vma=False
    )
```
